32 devices in a mesh: copies: 2 (over y), grid: 4 (over z), slab: 4 (over x, core).
Axes of the slice: x: 2, y: 2, z: 4, core: 2. Of those that a mesh axis runs over, the one named last changes fastest.
Arguments:
- field: float32 [8, 128, 64, 128], P(('copies', 'grid'), 'slab'), parts along dimension 0, may hold values from -6 to 6
- levels: int32 [8, 5], P(('copies', 'grid')), parts along dimension 0, may hold values from 1 to 3
- owner: int32 [256], P('copies'), parts along dimension 0, may hold values from 0 to 127, each once
Outputs:
- combined: float32 [256, 64, 128], P(('copies', 'grid'), 'slab'), parts along dimension 0
The draws below stay inside these ranges and needn't reach their ends.
There are 2 independent parts, one for each index of `copies`. The reference program is written for one: setup_inputs(seed, part) draws one part's arguments, and reference() takes and returns one part's arrays. A program takes and returns all parts, laid end to end along the dimension named above; each array names one. Nothing has to cross between parts.
All inputs are finite; a program needn't handle non-finite values.
Results may differ from the reference program's by a relative error of at most 0.0003.
Values sent between devices are 32-bit elements; how exact they have to be, the bound alone decides.
A program may use at most 64 MiB of HBM per device.

```python
import jax
import jax.numpy as jnp
import numpy as np
from jax import lax

N0 = 128
N1 = 2
N2 = 8
N3 = 4
N4 = 128
STEPS = 4
Q = 64
GRIDS = 4


def touch_ends(values, key, smallest, top_value):
    longest = values.shape.index(max(values.shape))
    spots = []
    for shift in (0, 1):
        where = [jax.random.randint(jax.random.fold_in(key, axis), (), 0, length) for axis, length in enumerate(values.shape)]
        where[longest] = (where[longest] + shift) % values.shape[longest]
        spots.append(tuple(where))
    return values.at[spots[0]].set(smallest).at[spots[1]].set(top_value)


def steps_of(own_key, extent, cuts, low, high):
    def one(axis_at, shards_of):
        steps = jax.random.uniform(jax.random.fold_in(jax.random.fold_in(own_key, 6), axis_at), (shards_of,), jnp.float32, low / len(cuts), high / len(cuts))
        return jnp.repeat(jnp.exp(steps), extent[axis_at] // shards_of).reshape((-1,) + (1,) * (len(extent) - axis_at - 1))

    loudness = one(*cuts[0])
    for cut in cuts[1:]:
        loudness = loudness * one(*cut)
    return loudness


def bell_draw(own_key, dims, width, most, cuts=(), held_as=jnp.bfloat16):
    loudness = steps_of(own_key, dims, cuts, -0.22, 0.18) if cuts else 1.0
    entries = jax.random.normal(own_key, dims, jnp.float32) * width * loudness
    return jnp.minimum(jnp.maximum(entries, -most), most).astype(held_as)


def setup_inputs(seed: int = 0, part: int = 0) -> dict:
    splits = jax.random.split(jax.random.key(seed), 4)
    part_splits = jax.random.split(jax.random.fold_in(splits[3], part), 4)
    return {
        "field": bell_draw(part_splits[0], (GRIDS, N0, Q, N4), 1.0, 6.0, ((0, 4), (1, 4)), jnp.float32),
        "levels": touch_ends(jax.random.randint(part_splits[1], (GRIDS, 5), 1, 4), jax.random.fold_in(part_splits[1], 1), 1, 3).astype(jnp.int32),
        "owner": jax.random.permutation(part_splits[2], N0).astype(jnp.int32),
    }


ADVECT = 0.08
DIFFUSE = 0.03

def build_tables(count):
    depth = count.bit_length() - 1
    matrix = np.eye(count)
    inverse = np.zeros((count, count))
    inverse[0, 0] = 1.0
    level_rows = np.zeros(count, np.int32)
    for index in range(1, count):
        zeros = (index & -index).bit_length() - 1
        spacing = 1 << zeros
        matrix[index, index - spacing] -= 0.5
        matrix[index, (index + spacing) % count] -= 0.5
        level_rows[index] = depth - zeros
    for zeros in range(depth - 1, -1, -1):
        spacing = 1 << zeros
        for index in range(spacing, count, 2 * spacing):
            inverse[index] = 0.5 * (inverse[index - spacing] + inverse[(index + spacing) % count])
            inverse[index, index] += 1.0
    return (matrix.astype(np.float32), inverse.astype(np.float32), level_rows)

def advance_full(state, scales):
    speed = 1.0 + 0.5 * jnp.tanh(state)
    change = jnp.zeros_like(state)
    for axis in range(5):
        back = jnp.roll(state, 1, axis)
        ahead = jnp.roll(state, -1, axis)
        change = change - ADVECT * scales[axis] * speed * (state - back) + DIFFUSE * scales[axis] ** 2 * (ahead - 2.0 * state + back)
    return state + change

def reference(field, levels, owner):
    matrix, inverse, level_rows = build_tables(N0)
    matrix = jnp.asarray(matrix).astype(jnp.float32)
    inverse = jnp.asarray(inverse).astype(jnp.float32)
    level_rows = jnp.asarray(level_rows).astype(jnp.int32)
    depth = N0.bit_length() - 1

    def keep_of(level_vec):
        return (level_rows <= depth - 3 + level_vec[0]).astype(jnp.float32)[:, None, None]

    def grid_terms(inputs):
        state, level_vec = inputs
        scales = jnp.exp2(level_vec.astype(jnp.float32)) / 8.0
        grid5 = state.reshape(N0, N1, N2, N3, N4)
        for step in range(STEPS):
            grid5 = advance_full(grid5, scales)
        hier = jnp.dot(matrix, grid5.reshape(N0, -1), precision=lax.Precision.HIGHEST).reshape(N0, Q, N4)
        weight = jnp.where(jnp.sum(level_vec) % 2 == 0, 1.0, -1.0).astype(jnp.float32) / jnp.sqrt(jnp.float32(GRIDS))
        return weight * keep_of(level_vec) * hier
    sums = lax.optimization_barrier(jnp.sum(lax.map(grid_terms, (field, levels)), axis=0))

    def restart(level_vec):
        masked = (keep_of(level_vec) * sums).reshape(N0, -1)
        return jnp.dot(inverse, masked, precision=lax.Precision.HIGHEST).reshape(N0, Q, N4)
    restarted = lax.map(restart, levels)
    sums = lax.optimization_barrier(jnp.sum(lax.map(grid_terms, (restarted, levels)), axis=0))
    return sums[owner]
```

```python
import functools
import math

import jax
import jax.numpy as jnp
from jax import lax
from jax.experimental import pallas as pl
from jax.experimental.pallas import tpu as pltpu
from jax.sharding import PartitionSpec as P

N1 = 2
N2 = 8
N3 = 4
STEPS = 4
SUB = 8
CHUNK = 2
LOW = STEPS
HIGH = STEPS + 1

ADVECT = 0.08
DIFFUSE = 0.03
MESH = pl.DeviceIdType.MESH


def advance_row(u, back0, ahead0, coef):
    adv, dif, adv_sum, dif_sum = coef
    tiles = u.shape[0]
    sub = lax.broadcasted_iota(jnp.int32, u.shape, 1)
    inner = sub % N3
    back3 = jnp.where(inner == 0, pltpu.roll(u, SUB - N3 + 1, 1), pltpu.roll(u, 1, 1))
    ahead3 = jnp.where(inner == N3 - 1, pltpu.roll(u, N3 - 1, 1), pltpu.roll(u, SUB - 1, 1))
    turned = pltpu.roll(u, N3, 1)
    half = tiles // N1
    parts = [turned[n * half:(n + 1) * half] for n in range(N1)]
    before = jnp.concatenate([x for p in parts for x in (p[half - 1:], p[:half - 1])], axis=0)
    after = jnp.concatenate([x for p in parts for x in (p[1:], p[:1])], axis=0)
    back2 = jnp.where(sub < N3, before, turned)
    ahead2 = jnp.where(sub < N3, turned, after)
    other = jnp.concatenate([u[half:], u[:half]], axis=0)
    back4 = pltpu.roll(u, 1, 2)
    ahead4 = pltpu.roll(u, u.shape[2] - 1, 2)
    upwind = (adv[0] * back0 + adv[1] * other + adv[2] * back2 + adv[3] * back3 + adv[4] * back4
              - adv_sum * u)
    spread = (dif[0] * (back0 + ahead0) + (2.0 * dif[1]) * other + dif[2] * (back2 + ahead2)
              + dif[3] * (back3 + ahead3) + dif[4] * (back4 + ahead4) - dif_sum * u)
    return u + (1.0 + 0.5 * jnp.tanh(u)) * upwind + spread


def kernel(sizes, par, owner, u_in, out, ext_a, ext_b, ext_s, terms, from_left, from_right,
           final, whole, rs_left, rs_right, rs_send,
           h_send, h_recv, up_send, l_recv, r_recv, dl_send, dr_send, d_recv, g_send, g_recv,
           a_send, a_recv, rs_ssem, rsl_recv, rsr_recv):
    Z, S, rows, count = sizes
    z = lax.axis_index("grid")
    s = lax.axis_index("slab")
    nxt, prv = lax.rem(s + 1, S), lax.rem(s + S - 1, S)
    ext = rows + LOW + HIGH
    chunks = rows // CHUNK
    pairs = chunks // 2
    tiles_out = whole.shape[1]
    owned = count // Z
    piece = rs_left.shape[2]
    pieces = owned // piece

    def remote(src, dst, ssem, rsem, **where):
        return pltpu.make_async_remote_copy(src_ref=src, dst_ref=dst, send_sem=ssem, recv_sem=rsem,
                                            device_id=where, device_id_type=MESH)

    adv = [par[d] for d in range(5)]
    dif = [par[5 + d] for d in range(5)]
    coef = (adv, dif, par[10], par[11])
    weight, keep_mid, keep_fine = par[12], par[13], par[14]

    barrier = pltpu.get_barrier_semaphore()
    for off in range(1, S):
        pl.semaphore_signal(barrier, inc=1, device_id={"slab": lax.rem(s + off, S)}, device_id_type=MESH)

    @pl.when(z > 0)
    def _():
        pl.semaphore_signal(barrier, inc=1, device_id={"grid": z - 1}, device_id_type=MESH)

    @pl.when(z < Z - 1)
    def _():
        pl.semaphore_signal(barrier, inc=1, device_id={"grid": z + 1}, device_id_type=MESH)

    pl.semaphore_wait(barrier, S - 1 + jnp.where(z > 0, 1, 0) + jnp.where(z < Z - 1, 1, 0))

    def run_rows(src, dst, low, high):
        @pl.loop(low, high)
        def _(e):
            dst[e] = advance_row(src[e], src[e - 1], src[e + 1], coef)

    def later_steps():
        run_rows(ext_b, ext_a, 2, ext - 2)
        run_rows(ext_a, ext_b, 3, ext - 3)
        run_rows(ext_b, ext_a, 4, ext - 4)

    def make_terms(dst):
        @pl.loop(0, rows // 4)
        def _(m):
            r = 4 * m
            u0, u1, u2, u3, u4 = [ext_a[LOW + r + k] for k in range(5)]
            dst[r] = weight * u0
            dst[r + 1] = (weight * keep_fine) * (u1 - 0.5 * (u0 + u2))
            dst[r + 2] = (weight * keep_mid) * (u2 - 0.5 * (u0 + u4))
            dst[r + 3] = (weight * keep_fine) * (u3 - 0.5 * (u2 + u4))

    up = remote(u_in.at[pl.ds(rows - LOW, LOW)], ext_a.at[pl.ds(0, LOW)], h_send.at[0], h_recv.at[0], slab=nxt)
    down = remote(u_in.at[pl.ds(0, HIGH)], ext_a.at[pl.ds(LOW + rows, HIGH)], h_send.at[1], h_recv.at[1], slab=prv)
    up.start()
    down.start()

    @pl.loop(0, rows)
    def _(r):
        ext_a[LOW + r] = u_in[r]

    run_rows(ext_a, ext_b, LOW + 1, LOW + rows - 1)
    up.wait()
    down.wait()
    run_rows(ext_a, ext_b, 1, LOW + 1)
    run_rows(ext_a, ext_b, LOW + rows - 1, ext - 1)
    later_steps()
    make_terms(terms)

    roots = (Z // 2 - 1, Z // 2)

    def at(position):
        return lax.rem(position + chunks - 2, chunks)

    def span(c):
        return pl.ds(c * CHUNK, CHUNK)

    def shifted(c):
        return pl.ds(LOW + c * CHUNK, CHUNK)

    def to_right(c):
        return remote(terms.at[span(c)], from_left.at[span(c)], up_send.at[c], l_recv.at[c], grid=lax.rem(z + 1, Z))

    def to_left(c):
        return remote(terms.at[span(c)], from_right.at[span(c)], up_send.at[c], r_recv.at[c],
                      grid=lax.rem(z + Z - 1, Z))

    def result_right(c):
        return remote(ext_s.at[shifted(c)], ext_s.at[shifted(c)], dr_send.at[c], d_recv.at[c], grid=lax.rem(z + 1, Z))

    def result_left(c):
        return remote(ext_s.at[shifted(c)], ext_s.at[shifted(c)], dl_send.at[c], d_recv.at[c],
                      grid=lax.rem(z + Z - 1, Z))

    def add_in(c, other):
        for k in range(CHUNK):
            terms[c * CHUNK + k] += other[c * CHUNK + k]

    def inward(c, root):
        @pl.when(z < root)
        def _():
            @pl.when(z > 0)
            def _():
                to_right(c).wait_recv()
                add_in(c, from_left)
            to_right(c).start()

        @pl.when(z > root)
        def _():
            @pl.when(z < Z - 1)
            def _():
                to_left(c).wait_recv()
                add_in(c, from_right)
            to_left(c).start()

    def at_root(c, root):
        @pl.when(z == root)
        def _():
            if root > 0:
                to_right(c).wait_recv()
                add_in(c, from_left)
            if root < Z - 1:
                to_left(c).wait_recv()
                add_in(c, from_right)
            for k in range(CHUNK):
                ext_s[LOW + c * CHUNK + k] = terms[c * CHUNK + k]
            if root > 0:
                result_left(c).start()
            if root < Z - 1:
                result_right(c).start()

    def outward(c, root):
        @pl.when(z < root)
        def _():
            result_right(c).wait_recv()

            @pl.when(z > 0)
            def _():
                result_left(c).start()

        @pl.when(z > root)
        def _():
            result_left(c).wait_recv()

            @pl.when(z < Z - 1)
            def _():
                result_right(c).start()

    halo_up = remote(ext_s.at[pl.ds(rows, LOW)], ext_s.at[pl.ds(0, LOW)], g_send.at[0], g_recv.at[0], slab=nxt)
    halo_down = remote(ext_s.at[pl.ds(LOW, HIGH)], ext_s.at[pl.ds(LOW + rows, HIGH)], g_send.at[1], g_recv.at[1],
                       slab=prv)
    root_lag, out_lag = 1, 2
    edge = out_lag + (4 + CHUNK + HIGH) // (2 * CHUNK)

    @pl.loop(0, pairs + out_lag)
    def _(j):
        @pl.when(j < pairs)
        def _():
            for k, root in enumerate(roots):
                inward(at(2 * j + k), root)

        @pl.when((j >= root_lag) & (j < pairs + root_lag))
        def _():
            for k, root in enumerate(roots):
                at_root(at(2 * (j - root_lag) + k), root)

        @pl.when(j >= out_lag)
        def _():
            for k, root in enumerate(roots):
                outward(at(2 * (j - out_lag) + k), root)

        @pl.when(j == edge)
        def _():
            halo_up.start()
            halo_down.start()

    def restart(low, high):
        @pl.loop(low, high)
        def _(m):
            e = 4 * m
            s0, s1, s2, s3, s4 = [ext_s[e + k] for k in range(5)]
            mid = 0.5 * (s0 + s4) + keep_mid * s2
            ext_a[e] = s0
            ext_a[e + 1] = 0.5 * (s0 + mid) + keep_fine * s1
            ext_a[e + 2] = mid
            ext_a[e + 3] = 0.5 * (mid + s4) + keep_fine * s3
            ext_a[e + 4] = s4

    halo_up.wait()
    halo_down.wait()
    restart(0, (ext - 1) // 4)
    run_rows(ext_a, ext_b, 1, ext - 1)
    later_steps()
    make_terms(final)

    def exchange(off):
        peer = lax.rem(s + off, S)
        return remote(final.at[:, pl.ds(peer * tiles_out, tiles_out)], whole.at[pl.ds(s * rows, rows)],
                      a_send.at[off - 1], a_recv.at[off - 1], slab=peer)

    def arrival(off):
        peer = lax.rem(s + S - off, S)
        return remote(final.at[:, pl.ds(peer * tiles_out, tiles_out)], whole.at[pl.ds(peer * rows, rows)],
                      a_send.at[off - 1], a_recv.at[off - 1], slab=peer)

    for off in range(1, S):
        exchange(off).start()

    @pl.loop(0, rows)
    def _(r):
        whole[s * rows + r] = final[r, pl.ds(s * tiles_out, tiles_out)]

    @pl.loop(0, chunks)
    def _(c):
        for k, root in enumerate(roots):
            @pl.when((lax.rem(c + 2, chunks) % 2 == k) & (z != root))
            def _():
                to_right(c).wait_send()

            @pl.when((lax.rem(c + 2, chunks) % 2 == k) & (z <= root) & (z > 0))
            def _():
                result_left(c).wait_send()

            @pl.when((lax.rem(c + 2, chunks) % 2 == k) & (z >= root) & (z < Z - 1))
            def _():
                result_right(c).wait_send()

    for off in range(1, S):
        arrival(off).wait_recv()
    for spacing in [1 << t for t in range(2, count.bit_length() - 1)]:
        for i in range(spacing, count, 2 * spacing):
            whole[i] = whole[i] - 0.5 * (whole[i - spacing] + whole[(i + spacing) % count])

    def rs_right_copy(k, p):
        return remote(rs_send.at[k, p], rs_left.at[k, p], rs_ssem.at[k, p], rsl_recv.at[k, p], grid=lax.rem(z + 1, Z))

    def rs_left_copy(k, p):
        return remote(rs_send.at[k, p], rs_right.at[k, p], rs_ssem.at[k, p], rsr_recv.at[k, p],
                      grid=lax.rem(z + Z - 1, Z))

    def own(k, p, r):
        return whole[owner[k * owned + p * piece + r]]

    @pl.loop(0, (Z - 1) * pieces)
    def _(j):
        p = j % pieces
        k = Z - 1 - j // pieces

        @pl.when(k > z)
        def _():
            @pl.loop(0, piece)
            def _(r):
                rs_send[k, p, r] = own(k, p, r)

            @pl.when(z > 0)
            def _():
                rs_right_copy(k, p).wait_recv()

                @pl.loop(0, piece)
                def _(r):
                    rs_send[k, p, r] += rs_left[k, p, r]
            rs_right_copy(k, p).start()

        n = j // pieces

        @pl.when(n < z)
        def _():
            @pl.loop(0, piece)
            def _(r):
                rs_send[n, p, r] = own(n, p, r)

            @pl.when(z < Z - 1)
            def _():
                rs_left_copy(n, p).wait_recv()

                @pl.loop(0, piece)
                def _(r):
                    rs_send[n, p, r] += rs_right[n, p, r]
            rs_left_copy(n, p).start()

    @pl.loop(0, pieces)
    def _(p):
        @pl.loop(0, piece)
        def _(r):
            out[p * piece + r] = own(z, p, r)

        @pl.when(z > 0)
        def _():
            rs_right_copy(z, p).wait_recv()

            @pl.loop(0, piece)
            def _(r):
                out[p * piece + r] += rs_left[z, p, r]

        @pl.when(z < Z - 1)
        def _():
            rs_left_copy(z, p).wait_recv()

            @pl.loop(0, piece)
            def _(r):
                out[p * piece + r] += rs_right[z, p, r]

    for off in range(1, S):
        exchange(off).wait_send()

    @pl.loop(0, Z)
    def _(k):
        @pl.when(k != z)
        def _():
            @pl.loop(0, pieces)
            def _(p):
                rs_right_copy(k, p).wait_send()


def local(field, levels, owner):
    _, rows, flat, lanes = field.shape
    Z, S = lax.axis_size("grid"), lax.axis_size("slab")
    count = owner.shape[0]
    tiles = flat // SUB
    tiles_out = tiles // S
    owned = count // Z
    piece = min(owned, 8)
    ext = rows + LOW + HIGH
    chunks = rows // CHUNK
    depth = count.bit_length() - 1
    vec = levels[0]
    scales = jnp.exp2(vec.astype(jnp.float32)) / 8.0
    adv = ADVECT * scales
    dif = DIFFUSE * scales ** 2
    weight = jnp.where(jnp.sum(vec) % 2 == 0, 1.0, -1.0) / math.sqrt(Z)
    kept = [(depth - t <= depth - 3 + vec[0]).astype(jnp.float32) for t in (1, 0)]
    par = jnp.concatenate([adv, dif, jnp.stack([jnp.sum(adv), 2.0 * jnp.sum(dif), weight.astype(jnp.float32), *kept])])
    u = field[0].reshape(rows, tiles, SUB, lanes)
    tail = (tiles, SUB, lanes)
    tail_out = (tiles_out, SUB, lanes)
    f32 = jnp.float32
    vmem = lambda *shape: pltpu.VMEM(shape, f32)
    sems = lambda *shape: pltpu.SemaphoreType.DMA(shape)
    pieces = owned // piece
    result = pl.pallas_call(
        functools.partial(kernel, (Z, S, rows, count)),
        out_shape=jax.ShapeDtypeStruct((owned,) + tail_out, f32),
        in_specs=[pl.BlockSpec(memory_space=pltpu.SMEM), pl.BlockSpec(memory_space=pltpu.SMEM),
                  pl.BlockSpec(memory_space=pltpu.VMEM)],
        out_specs=pl.BlockSpec(memory_space=pltpu.VMEM),
        scratch_shapes=[
            vmem(ext, *tail), vmem(ext, *tail), vmem(ext, *tail),
            vmem(rows, *tail), vmem(rows, *tail), vmem(rows, *tail),
            vmem(rows, *tail), vmem(count, *tail_out),
            vmem(Z, pieces, piece, *tail_out), vmem(Z, pieces, piece, *tail_out), vmem(Z, pieces, piece, *tail_out),
            sems(2), sems(2), sems(chunks), sems(chunks), sems(chunks), sems(chunks), sems(chunks), sems(chunks),
            sems(2), sems(2), sems(S - 1), sems(S - 1),
            sems(Z, pieces), sems(Z, pieces), sems(Z, pieces),
        ],
        compiler_params=pltpu.CompilerParams(collective_id=0, has_side_effects=True,
                                             vmem_limit_bytes=40 * 1024 * 1024),
    )(par, owner, u)
    return result.reshape(owned, flat // S, lanes)


def solution(mesh):
    in_specs = (P(("copies", "grid"), "slab", None, None), P(("copies", "grid"), None), P("copies"))
    out_specs = P(("copies", "grid"), "slab", None)
    return jax.shard_map(local, mesh=mesh, in_specs=in_specs, out_specs=out_specs, check_vma=False)
```

```python
import functools
import math

import jax
import jax.numpy as jnp
from jax import lax
from jax.experimental import pallas as pl
from jax.experimental.pallas import tpu as pltpu
from jax.sharding import PartitionSpec as P

N1 = 2
N2 = 8
N3 = 4
STEPS = 4
SUB = 8
CHUNK = 2
ROOT_LAG = 2
OUT_LAG = 5
RS_LAG = 2
LOW = STEPS
HIGH = STEPS + 1

ADVECT = 0.08
DIFFUSE = 0.03
MESH = pl.DeviceIdType.MESH


def advance_row(u, back0, ahead0, coef):
    adv, dif, adv_sum, dif_sum = coef
    tiles = u.shape[0]
    sub = lax.broadcasted_iota(jnp.int32, u.shape, 1)
    inner = sub % N3
    back3 = jnp.where(inner == 0, pltpu.roll(u, SUB - N3 + 1, 1), pltpu.roll(u, 1, 1))
    ahead3 = jnp.where(inner == N3 - 1, pltpu.roll(u, N3 - 1, 1), pltpu.roll(u, SUB - 1, 1))
    turned = pltpu.roll(u, N3, 1)
    half = tiles // N1
    parts = [turned[n * half:(n + 1) * half] for n in range(N1)]
    before = jnp.concatenate([x for p in parts for x in (p[half - 1:], p[:half - 1])], axis=0)
    after = jnp.concatenate([x for p in parts for x in (p[1:], p[:1])], axis=0)
    back2 = jnp.where(sub < N3, before, turned)
    ahead2 = jnp.where(sub < N3, turned, after)
    other = jnp.concatenate([u[half:], u[:half]], axis=0)
    back4 = pltpu.roll(u, 1, 2)
    ahead4 = pltpu.roll(u, u.shape[2] - 1, 2)
    upwind = (adv[0] * back0 + adv[1] * other + adv[2] * back2 + adv[3] * back3 + adv[4] * back4
              - adv_sum * u)
    spread = (dif[0] * (back0 + ahead0) + (2.0 * dif[1]) * other + dif[2] * (back2 + ahead2)
              + dif[3] * (back3 + ahead3) + dif[4] * (back4 + ahead4) - dif_sum * u)
    return u + (1.0 + 0.5 * jnp.tanh(u)) * upwind + spread


def kernel(sizes, levels, owner, u_in, out, ext_a, ext_b, ext_s, terms, from_left, from_right,
           final, whole, rs_left, rs_right, rs_send,
           h_send, h_recv, up_send, l_recv, r_recv, dl_send, dr_send, d_recv, g_send, g_recv,
           a_send, a_recv, rs_ssem, rsl_recv, rsr_recv, in_sem):
    Z, S, rows, count = sizes
    z = lax.axis_index("grid")
    s = lax.axis_index("slab")
    nxt, prv = lax.rem(s + 1, S), lax.rem(s + S - 1, S)
    ext = rows + LOW + HIGH
    chunks = rows // CHUNK
    pairs = chunks // 2
    tiles_out = whole.shape[1]
    owned = count // Z
    piece = rs_left.shape[2]
    pieces = owned // piece

    def remote(src, dst, ssem, rsem, **where):
        return pltpu.make_async_remote_copy(src_ref=src, dst_ref=dst, send_sem=ssem, recv_sem=rsem,
                                            device_id=where, device_id_type=MESH)

    loaded = pltpu.make_async_copy(u_in, ext_a.at[pl.ds(LOW, rows)], in_sem)
    loaded.start()
    vec = [levels[0, d] for d in range(5)]
    scales = [lax.shift_left(jnp.int32(1), v).astype(jnp.float32) * 0.125 for v in vec]
    adv = [ADVECT * x for x in scales]
    dif = [DIFFUSE * (x * x) for x in scales]
    coef = (adv, dif, sum(adv[1:], adv[0]), 2.0 * sum(dif[1:], dif[0]))
    size = jnp.float32(1.0 / math.sqrt(Z))
    weight = jnp.where(sum(vec[1:], vec[0]) % 2 == 0, size, -size)
    keep_mid, keep_fine = [jnp.where(3 - t <= vec[0], jnp.float32(1.0), jnp.float32(0.0)) for t in (1, 0)]

    barrier = pltpu.get_barrier_semaphore()
    for off in range(1, S):
        pl.semaphore_signal(barrier, inc=1, device_id={"slab": lax.rem(s + off, S)}, device_id_type=MESH)

    @pl.when(z > 0)
    def _():
        pl.semaphore_signal(barrier, inc=1, device_id={"grid": z - 1}, device_id_type=MESH)

    @pl.when(z < Z - 1)
    def _():
        pl.semaphore_signal(barrier, inc=1, device_id={"grid": z + 1}, device_id_type=MESH)

    pl.semaphore_wait(barrier, S - 1 + jnp.where(z > 0, 1, 0) + jnp.where(z < Z - 1, 1, 0))

    def run_rows(src, dst, low, high):
        @pl.loop(low, high)
        def _(e):
            dst[e] = advance_row(src[e], src[e - 1], src[e + 1], coef)

    def later_steps():
        run_rows(ext_b, ext_a, 2, ext - 2)
        run_rows(ext_a, ext_b, 3, ext - 3)
        run_rows(ext_b, ext_a, 4, ext - 4)

    def make_terms(dst):
        @pl.loop(0, rows // 4)
        def _(m):
            r = 4 * m
            u0, u1, u2, u3, u4 = [ext_a[LOW + r + k] for k in range(5)]
            dst[r] = weight * u0
            dst[r + 1] = (weight * keep_fine) * (u1 - 0.5 * (u0 + u2))
            dst[r + 2] = (weight * keep_mid) * (u2 - 0.5 * (u0 + u4))
            dst[r + 3] = (weight * keep_fine) * (u3 - 0.5 * (u2 + u4))

    up = remote(ext_a.at[pl.ds(rows, LOW)], ext_a.at[pl.ds(0, LOW)], h_send.at[0], h_recv.at[0], slab=nxt)
    loaded.wait()
    down = remote(ext_a.at[pl.ds(LOW, HIGH)], ext_a.at[pl.ds(LOW + rows, HIGH)], h_send.at[1], h_recv.at[1], slab=prv)
    up.start()
    down.start()

    run_rows(ext_a, ext_b, LOW + 1, LOW + rows - 1)
    up.wait()
    down.wait()
    run_rows(ext_a, ext_b, 1, LOW + 1)
    run_rows(ext_a, ext_b, LOW + rows - 1, ext - 1)
    later_steps()
    make_terms(terms)

    roots = (Z // 2 - 1, Z // 2)

    def at(position):
        return lax.rem(position + chunks - LOW // CHUNK, chunks)

    def span(c):
        return pl.ds(c * CHUNK, CHUNK)

    def shifted(c):
        return pl.ds(LOW + c * CHUNK, CHUNK)

    def to_right(c):
        return remote(terms.at[span(c)], from_left.at[span(c)], up_send.at[c], l_recv.at[c], grid=lax.rem(z + 1, Z))

    def to_left(c):
        return remote(terms.at[span(c)], from_right.at[span(c)], up_send.at[c], r_recv.at[c],
                      grid=lax.rem(z + Z - 1, Z))

    def result_right(c):
        return remote(ext_s.at[shifted(c)], ext_s.at[shifted(c)], dr_send.at[c], d_recv.at[c], grid=lax.rem(z + 1, Z))

    def result_left(c):
        return remote(ext_s.at[shifted(c)], ext_s.at[shifted(c)], dl_send.at[c], d_recv.at[c],
                      grid=lax.rem(z + Z - 1, Z))

    def add_in(c, other):
        for k in range(CHUNK):
            terms[c * CHUNK + k] += other[c * CHUNK + k]

    def inward(c, root):
        @pl.when(z < root)
        def _():
            @pl.when(z > 0)
            def _():
                to_right(c).wait_recv()
                add_in(c, from_left)
            to_right(c).start()

        @pl.when(z > root)
        def _():
            @pl.when(z < Z - 1)
            def _():
                to_left(c).wait_recv()
                add_in(c, from_right)
            to_left(c).start()

    def at_root(c, root):
        @pl.when(z == root)
        def _():
            if root > 0:
                to_right(c).wait_recv()
                add_in(c, from_left)
            if root < Z - 1:
                to_left(c).wait_recv()
                add_in(c, from_right)
            for k in range(CHUNK):
                ext_s[LOW + c * CHUNK + k] = terms[c * CHUNK + k]
            if root > 0:
                result_left(c).start()
            if root < Z - 1:
                result_right(c).start()

    def outward(c, root):
        @pl.when(z < root)
        def _():
            result_right(c).wait_recv()

            @pl.when(z > 0)
            def _():
                result_left(c).start()

        @pl.when(z > root)
        def _():
            result_left(c).wait_recv()

            @pl.when(z < Z - 1)
            def _():
                result_right(c).start()

    halo_up = remote(ext_s.at[pl.ds(rows, LOW)], ext_s.at[pl.ds(0, LOW)], g_send.at[0], g_recv.at[0], slab=nxt)
    halo_down = remote(ext_s.at[pl.ds(LOW, HIGH)], ext_s.at[pl.ds(LOW + rows, HIGH)], g_send.at[1], g_recv.at[1],
                       slab=prv)
    root_lag, out_lag = ROOT_LAG, OUT_LAG
    edge = out_lag + (LOW // CHUNK + -(-HIGH // CHUNK) - 1) // 2

    @pl.loop(0, pairs + out_lag)
    def _(j):
        @pl.when(j < pairs)
        def _():
            for k, root in enumerate(roots):
                inward(at(2 * j + k), root)

        @pl.when((j >= root_lag) & (j < pairs + root_lag))
        def _():
            for k, root in enumerate(roots):
                at_root(at(2 * (j - root_lag) + k), root)

        @pl.when(j >= out_lag)
        def _():
            for k, root in enumerate(roots):
                outward(at(2 * (j - out_lag) + k), root)

        @pl.when(j == edge)
        def _():
            halo_up.start()
            halo_down.start()

    def restart(low, high):
        @pl.loop(low, high)
        def _(m):
            e = 4 * m
            s0, s1, s2, s3, s4 = [ext_s[e + k] for k in range(5)]
            mid = 0.5 * (s0 + s4) + keep_mid * s2
            ext_a[e] = s0
            ext_a[e + 1] = 0.5 * (s0 + mid) + keep_fine * s1
            ext_a[e + 2] = mid
            ext_a[e + 3] = 0.5 * (mid + s4) + keep_fine * s3
            ext_a[e + 4] = s4

    halo_up.wait()
    halo_down.wait()
    restart(0, (ext - 1) // 4)
    run_rows(ext_a, ext_b, 1, ext - 1)
    later_steps()
    make_terms(final)

    def exchange(off):
        peer = lax.rem(s + off, S)
        return remote(final.at[:, pl.ds(peer * tiles_out, tiles_out)], whole.at[pl.ds(s * rows, rows)],
                      a_send.at[off - 1], a_recv.at[off - 1], slab=peer)

    def arrival(off):
        peer = lax.rem(s + S - off, S)
        return remote(final.at[:, pl.ds(peer * tiles_out, tiles_out)], whole.at[pl.ds(peer * rows, rows)],
                      a_send.at[off - 1], a_recv.at[off - 1], slab=peer)

    for off in range(1, S):
        exchange(off).start()

    @pl.loop(0, rows)
    def _(r):
        whole[s * rows + r] = final[r, pl.ds(s * tiles_out, tiles_out)]

    @pl.loop(0, chunks)
    def _(c):
        for k, root in enumerate(roots):
            @pl.when(((c + LOW // CHUNK) % 2 == k) & (z != root))
            def _():
                to_right(c).wait_send()

            @pl.when(((c + LOW // CHUNK) % 2 == k) & (z <= root) & (z > 0))
            def _():
                result_left(c).wait_send()

            @pl.when(((c + LOW // CHUNK) % 2 == k) & (z >= root) & (z < Z - 1))
            def _():
                result_right(c).wait_send()

    for off in range(1, S):
        arrival(off).wait_recv()
    for spacing in [1 << t for t in range(2, count.bit_length() - 1)]:
        for i in range(spacing, count, 2 * spacing):
            whole[i] = whole[i] - 0.5 * (whole[i - spacing] + whole[(i + spacing) % count])

    def rs_right_copy(k, p):
        return remote(rs_send.at[k, p], rs_left.at[k, p], rs_ssem.at[k, p], rsl_recv.at[k, p], grid=lax.rem(z + 1, Z))

    def rs_left_copy(k, p):
        return remote(rs_send.at[k, p], rs_right.at[k, p], rs_ssem.at[k, p], rsr_recv.at[k, p],
                      grid=lax.rem(z + Z - 1, Z))

    def own(k, p, r):
        return whole[owner[k * owned + p * piece + r]]

    steps = (Z - 1) * pieces

    @pl.loop(0, steps + (Z - 1) * RS_LAG)
    def _(j):
        jr = j - RS_LAG * z
        inside_r = (jr >= 0) & (jr < steps)
        jr = jnp.clip(jr, 0, steps - 1)
        p = jr % pieces
        k = Z - 1 - jr // pieces

        @pl.when(inside_r & (k > z))
        def _():
            @pl.loop(0, piece)
            def _(r):
                rs_send[k, p, r] = own(k, p, r)

            @pl.when(z > 0)
            def _():
                rs_right_copy(k, p).wait_recv()

                @pl.loop(0, piece)
                def _(r):
                    rs_send[k, p, r] += rs_left[k, p, r]
            rs_right_copy(k, p).start()

        jl = j - RS_LAG * (Z - 1 - z)
        inside_l = (jl >= 0) & (jl < steps)
        jl = jnp.clip(jl, 0, steps - 1)
        q = jl % pieces
        n = jl // pieces

        @pl.when(inside_l & (n < z))
        def _():
            @pl.loop(0, piece)
            def _(r):
                rs_send[n, q, r] = own(n, q, r)

            @pl.when(z < Z - 1)
            def _():
                rs_left_copy(n, q).wait_recv()

                @pl.loop(0, piece)
                def _(r):
                    rs_send[n, q, r] += rs_right[n, q, r]
            rs_left_copy(n, q).start()

    @pl.loop(0, pieces)
    def _(p):
        @pl.loop(0, piece)
        def _(r):
            out[p * piece + r] = own(z, p, r)

        @pl.when(z > 0)
        def _():
            rs_right_copy(z, p).wait_recv()

            @pl.loop(0, piece)
            def _(r):
                out[p * piece + r] += rs_left[z, p, r]

        @pl.when(z < Z - 1)
        def _():
            rs_left_copy(z, p).wait_recv()

            @pl.loop(0, piece)
            def _(r):
                out[p * piece + r] += rs_right[z, p, r]

    for off in range(1, S):
        exchange(off).wait_send()

    @pl.loop(0, Z)
    def _(k):
        @pl.when(k != z)
        def _():
            @pl.loop(0, pieces)
            def _(p):
                rs_right_copy(k, p).wait_send()


def local(field, levels, owner):
    _, rows, flat, lanes = field.shape
    Z, S = lax.axis_size("grid"), lax.axis_size("slab")
    count = owner.shape[0]
    tiles = flat // SUB
    tiles_out = tiles // S
    owned = count // Z
    piece = min(owned, 8)
    ext = rows + LOW + HIGH
    chunks = rows // CHUNK
    u = field[0].reshape(rows, tiles, SUB, lanes)
    tail = (tiles, SUB, lanes)
    tail_out = (tiles_out, SUB, lanes)
    f32 = jnp.float32
    vmem = lambda *shape: pltpu.VMEM(shape, f32)
    sems = lambda *shape: pltpu.SemaphoreType.DMA(shape)
    pieces = owned // piece
    result = pl.pallas_call(
        functools.partial(kernel, (Z, S, rows, count)),
        out_shape=jax.ShapeDtypeStruct((owned,) + tail_out, f32),
        in_specs=[pl.BlockSpec(memory_space=pltpu.SMEM), pl.BlockSpec(memory_space=pltpu.SMEM),
                  pl.BlockSpec(memory_space=pl.ANY)],
        out_specs=pl.BlockSpec(memory_space=pltpu.VMEM),
        scratch_shapes=[
            vmem(ext, *tail), vmem(ext, *tail), vmem(ext, *tail),
            vmem(rows, *tail), vmem(rows, *tail), vmem(rows, *tail),
            vmem(rows, *tail), vmem(count, *tail_out),
            vmem(Z, pieces, piece, *tail_out), vmem(Z, pieces, piece, *tail_out), vmem(Z, pieces, piece, *tail_out),
            sems(2), sems(2), sems(chunks), sems(chunks), sems(chunks), sems(chunks), sems(chunks), sems(chunks),
            sems(2), sems(2), sems(S - 1), sems(S - 1),
            sems(Z, pieces), sems(Z, pieces), sems(Z, pieces), pltpu.SemaphoreType.DMA,
        ],
        compiler_params=pltpu.CompilerParams(collective_id=0, has_side_effects=True,
                                             vmem_limit_bytes=40 * 1024 * 1024),
    )(levels, owner, u)
    return result.reshape(owned, flat // S, lanes)


def solution(mesh):
    in_specs = (P(("copies", "grid"), "slab", None, None), P(("copies", "grid"), None), P("copies"))
    out_specs = P(("copies", "grid"), "slab", None)
    return jax.shard_map(local, mesh=mesh, in_specs=in_specs, out_specs=out_specs, check_vma=False)
```

```python
import functools
import math

import jax
import jax.numpy as jnp
from jax import lax
from jax.experimental import pallas as pl
from jax.experimental.pallas import tpu as pltpu
from jax.sharding import PartitionSpec as P

N1 = 2
N2 = 8
N3 = 4
STEPS = 4
SUB = 8
CHUNK = 2
ROOT_LAG = 2
OUT_LAG = 5
RS_LAG = 2
WAVE_LAG = 4
LOW = STEPS
HIGH = STEPS + 1

ADVECT = 0.08
DIFFUSE = 0.03
MESH = pl.DeviceIdType.MESH


def advance_row(u, back0, ahead0, coef):
    adv, dif, adv_sum, dif_sum = coef
    tiles = u.shape[0]
    sub = lax.broadcasted_iota(jnp.int32, u.shape, 1)
    inner = sub % N3
    back3 = jnp.where(inner == 0, pltpu.roll(u, SUB - N3 + 1, 1), pltpu.roll(u, 1, 1))
    ahead3 = jnp.where(inner == N3 - 1, pltpu.roll(u, N3 - 1, 1), pltpu.roll(u, SUB - 1, 1))
    turned = pltpu.roll(u, N3, 1)
    half = tiles // N1
    parts = [turned[n * half:(n + 1) * half] for n in range(N1)]
    before = jnp.concatenate([x for p in parts for x in (p[half - 1:], p[:half - 1])], axis=0)
    after = jnp.concatenate([x for p in parts for x in (p[1:], p[:1])], axis=0)
    back2 = jnp.where(sub < N3, before, turned)
    ahead2 = jnp.where(sub < N3, turned, after)
    other = jnp.concatenate([u[half:], u[:half]], axis=0)
    back4 = pltpu.roll(u, 1, 2)
    ahead4 = pltpu.roll(u, u.shape[2] - 1, 2)
    upwind = (adv[0] * back0 + adv[1] * other + adv[2] * back2 + adv[3] * back3 + adv[4] * back4
              - adv_sum * u)
    spread = (dif[0] * (back0 + ahead0) + (2.0 * dif[1]) * other + dif[2] * (back2 + ahead2)
              + dif[3] * (back3 + ahead3) + dif[4] * (back4 + ahead4) - dif_sum * u)
    return u + (1.0 + 0.5 * jnp.tanh(u)) * upwind + spread


def kernel(sizes, levels, owner, u_in, out, first, second, ext_s, terms, from_left, from_right,
           final, whole, rs_left, rs_right, rs_send,
           h_send, h_recv, up_send, l_recv, r_recv, dl_send, dr_send, d_recv, g_send, g_recv,
           a_send, a_recv, rs_ssem, rsl_recv, rsr_recv, in_sem):
    Z, S, rows, count = sizes
    z = lax.axis_index("grid")
    s = lax.axis_index("slab")
    nxt, prv = lax.rem(s + 1, S), lax.rem(s + S - 1, S)
    ext = rows + LOW + HIGH
    chunks = rows // CHUNK
    pairs = chunks // 2
    tiles_out = whole.shape[1]
    owned = count // Z
    piece = rs_left.shape[2]
    pieces = owned // piece

    def remote(src, dst, ssem, rsem, **where):
        return pltpu.make_async_remote_copy(src_ref=src, dst_ref=dst, send_sem=ssem, recv_sem=rsem,
                                            device_id=where, device_id_type=MESH)

    groups = rows // 4
    loaded = pltpu.make_async_copy(u_in, first.at[0, pl.ds(LOW, rows)], in_sem)
    loaded.start()
    vec = [levels[0, d] for d in range(5)]
    scales = [lax.shift_left(jnp.int32(1), v).astype(jnp.float32) * 0.125 for v in vec]
    adv = [ADVECT * x for x in scales]
    dif = [DIFFUSE * (x * x) for x in scales]
    coef = (adv, dif, sum(adv[1:], adv[0]), 2.0 * sum(dif[1:], dif[0]))
    size = jnp.float32(1.0 / math.sqrt(Z))
    weight = jnp.where(sum(vec[1:], vec[0]) % 2 == 0, size, -size)
    keep_mid, keep_fine = [jnp.where(3 - t <= vec[0], jnp.float32(1.0), jnp.float32(0.0)) for t in (1, 0)]

    barrier = pltpu.get_barrier_semaphore()
    for off in range(1, S):
        pl.semaphore_signal(barrier, inc=1, device_id={"slab": lax.rem(s + off, S)}, device_id_type=MESH)

    @pl.when(z > 0)
    def _():
        pl.semaphore_signal(barrier, inc=1, device_id={"grid": z - 1}, device_id_type=MESH)

    @pl.when(z < Z - 1)
    def _():
        pl.semaphore_signal(barrier, inc=1, device_id={"grid": z + 1}, device_id_type=MESH)

    pl.semaphore_wait(barrier, S - 1 + jnp.where(z > 0, 1, 0) + jnp.where(z < Z - 1, 1, 0))

    def wave(bufs, g, fresh):
        for k in range(1, STEPS + 1):
            low = jnp.where(fresh, 4 * g + k, 4 * g + 9 - k)

            @pl.loop(low, 4 * g + 13 - k)
            def _(e):
                bufs[k, e] = advance_row(bufs[k - 1, e], bufs[k - 1, e - 1], bufs[k - 1, e + 1], coef)

    def make_terms(bufs, g, dst):
        r = 4 * g
        u0, u1, u2, u3, u4 = [bufs[STEPS, LOW + r + k] for k in range(5)]
        dst[r] = weight * u0
        dst[r + 1] = (weight * keep_fine) * (u1 - 0.5 * (u0 + u2))
        dst[r + 2] = (weight * keep_mid) * (u2 - 0.5 * (u0 + u4))
        dst[r + 3] = (weight * keep_fine) * (u3 - 0.5 * (u2 + u4))

    up = remote(first.at[0, pl.ds(rows, LOW)], first.at[0, pl.ds(0, LOW)], h_send.at[0], h_recv.at[0], slab=nxt)
    loaded.wait()
    down = remote(first.at[0, pl.ds(LOW, HIGH)], first.at[0, pl.ds(LOW + rows, HIGH)], h_send.at[1], h_recv.at[1], slab=prv)
    up.start()
    down.start()

    up.wait()
    down.wait()

    roots = (Z // 2 - 1, Z // 2)

    def at(position):
        return lax.rem(position + chunks - LOW // CHUNK, chunks)

    def span(c):
        return pl.ds(c * CHUNK, CHUNK)

    def shifted(c):
        return pl.ds(LOW + c * CHUNK, CHUNK)

    def to_right(c):
        return remote(terms.at[span(c)], from_left.at[span(c)], up_send.at[c], l_recv.at[c], grid=lax.rem(z + 1, Z))

    def to_left(c):
        return remote(terms.at[span(c)], from_right.at[span(c)], up_send.at[c], r_recv.at[c],
                      grid=lax.rem(z + Z - 1, Z))

    def result_right(c):
        return remote(ext_s.at[shifted(c)], ext_s.at[shifted(c)], dr_send.at[c], d_recv.at[c], grid=lax.rem(z + 1, Z))

    def result_left(c):
        return remote(ext_s.at[shifted(c)], ext_s.at[shifted(c)], dl_send.at[c], d_recv.at[c],
                      grid=lax.rem(z + Z - 1, Z))

    def add_in(c, other):
        for k in range(CHUNK):
            terms[c * CHUNK + k] += other[c * CHUNK + k]

    def inward(c, root):
        @pl.when(z < root)
        def _():
            @pl.when(z > 0)
            def _():
                to_right(c).wait_recv()
                add_in(c, from_left)
            to_right(c).start()

        @pl.when(z > root)
        def _():
            @pl.when(z < Z - 1)
            def _():
                to_left(c).wait_recv()
                add_in(c, from_right)
            to_left(c).start()

    def at_root(c, root):
        @pl.when(z == root)
        def _():
            if root > 0:
                to_right(c).wait_recv()
                add_in(c, from_left)
            if root < Z - 1:
                to_left(c).wait_recv()
                add_in(c, from_right)
            for k in range(CHUNK):
                ext_s[LOW + c * CHUNK + k] = terms[c * CHUNK + k]
            if root > 0:
                result_left(c).start()
            if root < Z - 1:
                result_right(c).start()

    def outward(c, root):
        @pl.when(z < root)
        def _():
            result_right(c).wait_recv()

            @pl.when(z > 0)
            def _():
                result_left(c).start()

        @pl.when(z > root)
        def _():
            result_left(c).wait_recv()

            @pl.when(z < Z - 1)
            def _():
                result_right(c).start()

    halo_up = remote(ext_s.at[pl.ds(rows, LOW)], ext_s.at[pl.ds(0, LOW)], g_send.at[0], g_recv.at[0], slab=nxt)
    halo_down = remote(ext_s.at[pl.ds(LOW, HIGH)], ext_s.at[pl.ds(LOW + rows, HIGH)], g_send.at[1], g_recv.at[1],
                       slab=prv)
    root_lag, out_lag = ROOT_LAG, OUT_LAG
    edge = out_lag + (LOW // CHUNK + -(-HIGH // CHUNK) - 1) // 2

    def restart(m):
        e = 4 * m
        s0, s1, s2, s3, s4 = [ext_s[e + k] for k in range(5)]
        mid = 0.5 * (s0 + s4) + keep_mid * s2
        second[0, e] = s0
        second[0, e + 1] = 0.5 * (s0 + mid) + keep_fine * s1
        second[0, e + 2] = mid
        second[0, e + 3] = 0.5 * (mid + s4) + keep_fine * s3
        second[0, e + 4] = s4

    def exchange(off, g):
        peer = lax.rem(s + off, S)
        return remote(final.at[pl.ds(4 * g, 4), pl.ds(peer * tiles_out, tiles_out)],
                      whole.at[pl.ds(s * rows + 4 * g, 4)],
                      a_send.at[off - 1, g], a_recv.at[off - 1, g], slab=peer)

    def arrival(off, g):
        peer = lax.rem(s + S - off, S)
        return remote(final.at[pl.ds(4 * g, 4), pl.ds(peer * tiles_out, tiles_out)],
                      whole.at[pl.ds(peer * rows + 4 * g, 4)],
                      a_send.at[off - 1, g], a_recv.at[off - 1, g], slab=peer)

    last = pairs + out_lag
    wave_lag = out_lag + WAVE_LAG

    @pl.loop(0, max(last, groups + wave_lag))
    def _(j):
        @pl.when(j < pairs)
        def _():
            g = lax.rem(j + groups - 1, groups)
            wave(first, g, j < 2)
            make_terms(first, g, terms)
            for k, root in enumerate(roots):
                inward(at(2 * j + k), root)

        @pl.when((j >= root_lag) & (j < pairs + root_lag))
        def _():
            for k, root in enumerate(roots):
                at_root(at(2 * (j - root_lag) + k), root)

        @pl.when((j >= out_lag) & (j < last))
        def _():
            for k, root in enumerate(roots):
                outward(at(2 * (j - out_lag) + k), root)

        @pl.when(j == edge)
        def _():
            halo_up.start()
            halo_down.start()

        @pl.when(j == wave_lag)
        def _():
            halo_up.wait()
            halo_down.wait()
            restart(0)
            restart(1)

        @pl.when((j >= wave_lag) & (j < groups + wave_lag))
        def _():
            g = j - wave_lag
            restart(g + 2)
            wave(second, g, g == 0)
            make_terms(second, g, final)
            for off in range(1, S):
                exchange(off, g).start()
            for k in range(4):
                whole[s * rows + 4 * g + k] = final[4 * g + k, pl.ds(s * tiles_out, tiles_out)]

    @pl.loop(0, chunks)
    def _(c):
        for k, root in enumerate(roots):
            @pl.when(((c + LOW // CHUNK) % 2 == k) & (z != root))
            def _():
                to_right(c).wait_send()

            @pl.when(((c + LOW // CHUNK) % 2 == k) & (z <= root) & (z > 0))
            def _():
                result_left(c).wait_send()

            @pl.when(((c + LOW // CHUNK) % 2 == k) & (z >= root) & (z < Z - 1))
            def _():
                result_right(c).wait_send()

    @pl.loop(0, groups)
    def _(g):
        for off in range(1, S):
            arrival(off, g).wait_recv()

    for spacing in [1 << t for t in range(2, count.bit_length() - 1)]:
        for i in range(spacing, count, 2 * spacing):
            whole[i] = whole[i] - 0.5 * (whole[i - spacing] + whole[(i + spacing) % count])

    def rs_right_copy(k, p):
        return remote(rs_send.at[k, p], rs_left.at[k, p], rs_ssem.at[k, p], rsl_recv.at[k, p], grid=lax.rem(z + 1, Z))

    def rs_left_copy(k, p):
        return remote(rs_send.at[k, p], rs_right.at[k, p], rs_ssem.at[k, p], rsr_recv.at[k, p],
                      grid=lax.rem(z + Z - 1, Z))

    def own(k, p, r):
        return whole[owner[k * owned + p * piece + r]]

    steps = (Z - 1) * pieces

    @pl.loop(0, steps + (Z - 1) * RS_LAG)
    def _(j):
        jr = j - RS_LAG * z
        inside_r = (jr >= 0) & (jr < steps)
        jr = jnp.clip(jr, 0, steps - 1)
        p = jr % pieces
        k = Z - 1 - jr // pieces

        @pl.when(inside_r & (k > z))
        def _():
            @pl.loop(0, piece)
            def _(r):
                rs_send[k, p, r] = own(k, p, r)

            @pl.when(z > 0)
            def _():
                rs_right_copy(k, p).wait_recv()

                @pl.loop(0, piece)
                def _(r):
                    rs_send[k, p, r] += rs_left[k, p, r]
            rs_right_copy(k, p).start()

        jl = j - RS_LAG * (Z - 1 - z)
        inside_l = (jl >= 0) & (jl < steps)
        jl = jnp.clip(jl, 0, steps - 1)
        q = jl % pieces
        n = jl // pieces

        @pl.when(inside_l & (n < z))
        def _():
            @pl.loop(0, piece)
            def _(r):
                rs_send[n, q, r] = own(n, q, r)

            @pl.when(z < Z - 1)
            def _():
                rs_left_copy(n, q).wait_recv()

                @pl.loop(0, piece)
                def _(r):
                    rs_send[n, q, r] += rs_right[n, q, r]
            rs_left_copy(n, q).start()

    @pl.loop(0, pieces)
    def _(p):
        @pl.loop(0, piece)
        def _(r):
            out[p * piece + r] = own(z, p, r)

        @pl.when(z > 0)
        def _():
            rs_right_copy(z, p).wait_recv()

            @pl.loop(0, piece)
            def _(r):
                out[p * piece + r] += rs_left[z, p, r]

        @pl.when(z < Z - 1)
        def _():
            rs_left_copy(z, p).wait_recv()

            @pl.loop(0, piece)
            def _(r):
                out[p * piece + r] += rs_right[z, p, r]

    @pl.loop(0, groups)
    def _(g):
        for off in range(1, S):
            exchange(off, g).wait_send()

    @pl.loop(0, Z)
    def _(k):
        @pl.when(k != z)
        def _():
            @pl.loop(0, pieces)
            def _(p):
                rs_right_copy(k, p).wait_send()


def local(field, levels, owner):
    _, rows, flat, lanes = field.shape
    Z, S = lax.axis_size("grid"), lax.axis_size("slab")
    count = owner.shape[0]
    tiles = flat // SUB
    tiles_out = tiles // S
    owned = count // Z
    piece = min(owned, 8)
    ext = rows + LOW + HIGH
    chunks = rows // CHUNK
    u = field[0].reshape(rows, tiles, SUB, lanes)
    tail = (tiles, SUB, lanes)
    tail_out = (tiles_out, SUB, lanes)
    f32 = jnp.float32
    vmem = lambda *shape: pltpu.VMEM(shape, f32)
    sems = lambda *shape: pltpu.SemaphoreType.DMA(shape)
    pieces = owned // piece
    result = pl.pallas_call(
        functools.partial(kernel, (Z, S, rows, count)),
        out_shape=jax.ShapeDtypeStruct((owned,) + tail_out, f32),
        in_specs=[pl.BlockSpec(memory_space=pltpu.SMEM), pl.BlockSpec(memory_space=pltpu.SMEM),
                  pl.BlockSpec(memory_space=pl.ANY)],
        out_specs=pl.BlockSpec(memory_space=pltpu.VMEM),
        scratch_shapes=[
            vmem(STEPS + 1, ext, *tail), vmem(STEPS + 1, ext, *tail), vmem(ext, *tail),
            vmem(rows, *tail), vmem(rows, *tail), vmem(rows, *tail),
            vmem(rows, *tail), vmem(count, *tail_out),
            vmem(Z, pieces, piece, *tail_out), vmem(Z, pieces, piece, *tail_out), vmem(Z, pieces, piece, *tail_out),
            sems(2), sems(2), sems(chunks), sems(chunks), sems(chunks), sems(chunks), sems(chunks), sems(chunks),
            sems(2), sems(2), sems(S - 1, rows // 4), sems(S - 1, rows // 4),
            sems(Z, pieces), sems(Z, pieces), sems(Z, pieces), pltpu.SemaphoreType.DMA,
        ],
        compiler_params=pltpu.CompilerParams(collective_id=0, has_side_effects=True,
                                             vmem_limit_bytes=40 * 1024 * 1024),
    )(levels, owner, u)
    return result.reshape(owned, flat // S, lanes)


def solution(mesh):
    in_specs = (P(("copies", "grid"), "slab", None, None), P(("copies", "grid"), None), P("copies"))
    out_specs = P(("copies", "grid"), "slab", None)
    return jax.shard_map(local, mesh=mesh, in_specs=in_specs, out_specs=out_specs, check_vma=False)
```

```python
import functools
import math

import jax
import jax.numpy as jnp
from jax import lax
from jax.experimental import pallas as pl
from jax.experimental.pallas import tpu as pltpu
from jax.sharding import PartitionSpec as P

N1 = 2
N2 = 8
N3 = 4
STEPS = 4
SUB = 8
CHUNK = 2
ROOT_LAG = 3
OUT_LAG = 7
RS_LAG = 2
WAVE_LAG = 3
LOW = STEPS
HIGH = STEPS + 1

ADVECT = 0.08
DIFFUSE = 0.03
MESH = pl.DeviceIdType.MESH


def advance_row(u, back0, ahead0, coef):
    adv, dif, adv_sum, dif_sum = coef
    tiles = u.shape[0]
    sub = lax.broadcasted_iota(jnp.int32, u.shape, 1)
    inner = sub % N3
    back3 = jnp.where(inner == 0, pltpu.roll(u, SUB - N3 + 1, 1), pltpu.roll(u, 1, 1))
    ahead3 = jnp.where(inner == N3 - 1, pltpu.roll(u, N3 - 1, 1), pltpu.roll(u, SUB - 1, 1))
    turned = pltpu.roll(u, N3, 1)
    half = tiles // N1
    parts = [turned[n * half:(n + 1) * half] for n in range(N1)]
    before = jnp.concatenate([x for p in parts for x in (p[half - 1:], p[:half - 1])], axis=0)
    after = jnp.concatenate([x for p in parts for x in (p[1:], p[:1])], axis=0)
    back2 = jnp.where(sub < N3, before, turned)
    ahead2 = jnp.where(sub < N3, turned, after)
    other = jnp.concatenate([u[half:], u[:half]], axis=0)
    back4 = pltpu.roll(u, 1, 2)
    ahead4 = pltpu.roll(u, u.shape[2] - 1, 2)
    upwind = (adv[0] * back0 + adv[1] * other + adv[2] * back2 + adv[3] * back3 + adv[4] * back4
              - adv_sum * u)
    spread = (dif[0] * (back0 + ahead0) + (2.0 * dif[1]) * other + dif[2] * (back2 + ahead2)
              + dif[3] * (back3 + ahead3) + dif[4] * (back4 + ahead4) - dif_sum * u)
    return u + (1.0 + 0.5 * jnp.tanh(u)) * upwind + spread


def kernel(sizes, levels, owner, u_in, out, first, second, ext_s, terms, from_left, from_right,
           final, whole, rs_left, rs_right, rs_send,
           h_send, h_recv, up_send, l_recv, r_recv, dl_send, dr_send, d_recv, g_send, g_recv,
           a_send, a_recv, rs_ssem, rsl_recv, rsr_recv, in_sem):
    Z, S, rows, count = sizes
    z = lax.axis_index("grid")
    s = lax.axis_index("slab")
    nxt, prv = lax.rem(s + 1, S), lax.rem(s + S - 1, S)
    ext = rows + LOW + HIGH
    chunks = rows // CHUNK
    pairs = chunks // 2
    tiles_out = whole.shape[1]
    owned = count // Z
    piece = rs_left.shape[2]
    pieces = owned // piece

    def remote(src, dst, ssem, rsem, **where):
        return pltpu.make_async_remote_copy(src_ref=src, dst_ref=dst, send_sem=ssem, recv_sem=rsem,
                                            device_id=where, device_id_type=MESH)

    groups = rows // 4
    loaded = pltpu.make_async_copy(u_in, first.at[0, pl.ds(LOW, rows)], in_sem)
    loaded.start()
    vec = [levels[0, d] for d in range(5)]
    scales = [lax.shift_left(jnp.int32(1), v).astype(jnp.float32) * 0.125 for v in vec]
    adv = [ADVECT * x for x in scales]
    dif = [DIFFUSE * (x * x) for x in scales]
    coef = (adv, dif, sum(adv[1:], adv[0]), 2.0 * sum(dif[1:], dif[0]))
    size = jnp.float32(1.0 / math.sqrt(Z))
    weight = jnp.where(sum(vec[1:], vec[0]) % 2 == 0, size, -size)
    keep_mid, keep_fine = [jnp.where(3 - t <= vec[0], jnp.float32(1.0), jnp.float32(0.0)) for t in (1, 0)]

    barrier = pltpu.get_barrier_semaphore()
    for off in range(1, S):
        pl.semaphore_signal(barrier, inc=1, device_id={"slab": lax.rem(s + off, S)}, device_id_type=MESH)

    @pl.when(z > 0)
    def _():
        pl.semaphore_signal(barrier, inc=1, device_id={"grid": z - 1}, device_id_type=MESH)

    @pl.when(z < Z - 1)
    def _():
        pl.semaphore_signal(barrier, inc=1, device_id={"grid": z + 1}, device_id_type=MESH)

    pl.semaphore_wait(barrier, S - 1 + jnp.where(z > 0, 1, 0) + jnp.where(z < Z - 1, 1, 0))

    def wave(bufs, g, fresh):
        for k in range(1, STEPS + 1):
            low = jnp.where(fresh, 4 * g + k, 4 * g + 9 - k)

            @pl.loop(low, 4 * g + 9 - k)
            def _(e):
                bufs[k, e] = advance_row(bufs[k - 1, e], bufs[k - 1, e - 1], bufs[k - 1, e + 1], coef)

            @pl.loop(0, 2)
            def _(n):
                for e in [4 * g + 9 - k + 2 * n + i for i in range(2)]:
                    bufs[k, e] = advance_row(bufs[k - 1, e], bufs[k - 1, e - 1], bufs[k - 1, e + 1], coef)

    def make_terms(bufs, g, dst):
        r = 4 * g
        u0, u1, u2, u3, u4 = [bufs[STEPS, LOW + r + k] for k in range(5)]
        dst[r] = weight * u0
        dst[r + 1] = (weight * keep_fine) * (u1 - 0.5 * (u0 + u2))
        dst[r + 2] = (weight * keep_mid) * (u2 - 0.5 * (u0 + u4))
        dst[r + 3] = (weight * keep_fine) * (u3 - 0.5 * (u2 + u4))

    up = remote(first.at[0, pl.ds(rows, LOW)], first.at[0, pl.ds(0, LOW)], h_send.at[0], h_recv.at[0], slab=nxt)
    loaded.wait()
    down = remote(first.at[0, pl.ds(LOW, HIGH)], first.at[0, pl.ds(LOW + rows, HIGH)], h_send.at[1], h_recv.at[1], slab=prv)
    up.start()
    down.start()

    up.wait()
    down.wait()

    roots = (Z // 2 - 1, Z // 2)

    def at(position):
        return lax.rem(position + chunks - LOW // CHUNK, chunks)

    def span(c):
        return pl.ds(c * CHUNK, CHUNK)

    def shifted(c):
        return pl.ds(LOW + c * CHUNK, CHUNK)

    def to_right(c):
        return remote(terms.at[span(c)], from_left.at[span(c)], up_send.at[c], l_recv.at[c], grid=lax.rem(z + 1, Z))

    def to_left(c):
        return remote(terms.at[span(c)], from_right.at[span(c)], up_send.at[c], r_recv.at[c],
                      grid=lax.rem(z + Z - 1, Z))

    def result_right(c):
        return remote(ext_s.at[shifted(c)], ext_s.at[shifted(c)], dr_send.at[c], d_recv.at[c], grid=lax.rem(z + 1, Z))

    def result_left(c):
        return remote(ext_s.at[shifted(c)], ext_s.at[shifted(c)], dl_send.at[c], d_recv.at[c],
                      grid=lax.rem(z + Z - 1, Z))

    def add_in(c, other):
        for k in range(CHUNK):
            terms[c * CHUNK + k] += other[c * CHUNK + k]

    def inward(c, root):
        @pl.when(z < root)
        def _():
            @pl.when(z > 0)
            def _():
                to_right(c).wait_recv()
                add_in(c, from_left)
            to_right(c).start()

        @pl.when(z > root)
        def _():
            @pl.when(z < Z - 1)
            def _():
                to_left(c).wait_recv()
                add_in(c, from_right)
            to_left(c).start()

    def at_root(c, root):
        @pl.when(z == root)
        def _():
            if root > 0:
                to_right(c).wait_recv()
                add_in(c, from_left)
            if root < Z - 1:
                to_left(c).wait_recv()
                add_in(c, from_right)
            for k in range(CHUNK):
                ext_s[LOW + c * CHUNK + k] = terms[c * CHUNK + k]
            if root > 0:
                result_left(c).start()
            if root < Z - 1:
                result_right(c).start()

    def outward(c, root):
        @pl.when(z < root)
        def _():
            result_right(c).wait_recv()

            @pl.when(z > 0)
            def _():
                result_left(c).start()

        @pl.when(z > root)
        def _():
            result_left(c).wait_recv()

            @pl.when(z < Z - 1)
            def _():
                result_right(c).start()

    halo_up = remote(ext_s.at[pl.ds(rows, LOW)], ext_s.at[pl.ds(0, LOW)], g_send.at[0], g_recv.at[0], slab=nxt)
    halo_down = remote(ext_s.at[pl.ds(LOW, HIGH)], ext_s.at[pl.ds(LOW + rows, HIGH)], g_send.at[1], g_recv.at[1],
                       slab=prv)
    root_lag, out_lag = ROOT_LAG, OUT_LAG
    edge = out_lag + (LOW // CHUNK + -(-HIGH // CHUNK) - 1) // 2

    def restart(m):
        e = 4 * m
        s0, s1, s2, s3, s4 = [ext_s[e + k] for k in range(5)]
        mid = 0.5 * (s0 + s4) + keep_mid * s2
        second[0, e] = s0
        second[0, e + 1] = 0.5 * (s0 + mid) + keep_fine * s1
        second[0, e + 2] = mid
        second[0, e + 3] = 0.5 * (mid + s4) + keep_fine * s3
        second[0, e + 4] = s4

    def exchange(off, g):
        peer = lax.rem(s + off, S)
        return remote(final.at[pl.ds(4 * g, 4), pl.ds(peer * tiles_out, tiles_out)],
                      whole.at[pl.ds(s * rows + 4 * g, 4)],
                      a_send.at[off - 1, g], a_recv.at[off - 1, g], slab=peer)

    def arrival(off, g):
        peer = lax.rem(s + S - off, S)
        return remote(final.at[pl.ds(4 * g, 4), pl.ds(peer * tiles_out, tiles_out)],
                      whole.at[pl.ds(peer * rows + 4 * g, 4)],
                      a_send.at[off - 1, g], a_recv.at[off - 1, g], slab=peer)

    last = pairs + out_lag
    wave_lag = out_lag + WAVE_LAG

    @pl.loop(0, max(last, groups + wave_lag))
    def _(j):
        @pl.when(j < pairs)
        def _():
            g = lax.rem(j + groups - 1, groups)
            wave(first, g, j < 2)
            make_terms(first, g, terms)
            for k, root in enumerate(roots):
                inward(at(2 * j + k), root)

        @pl.when((j >= root_lag) & (j < pairs + root_lag))
        def _():
            for k, root in enumerate(roots):
                at_root(at(2 * (j - root_lag) + k), root)

        @pl.when((j >= out_lag) & (j < last))
        def _():
            for k, root in enumerate(roots):
                outward(at(2 * (j - out_lag) + k), root)

        @pl.when(j == edge)
        def _():
            halo_up.start()
            halo_down.start()

        @pl.when(j == wave_lag)
        def _():
            halo_up.wait()
            halo_down.wait()
            restart(0)
            restart(1)

        @pl.when((j >= wave_lag) & (j < groups + wave_lag))
        def _():
            g = j - wave_lag
            restart(g + 2)
            wave(second, g, g == 0)
            make_terms(second, g, final)
            for off in range(1, S):
                exchange(off, g).start()
            for k in range(4):
                whole[s * rows + 4 * g + k] = final[4 * g + k, pl.ds(s * tiles_out, tiles_out)]

    @pl.loop(0, chunks)
    def _(c):
        for k, root in enumerate(roots):
            @pl.when(((c + LOW // CHUNK) % 2 == k) & (z != root))
            def _():
                to_right(c).wait_send()

            @pl.when(((c + LOW // CHUNK) % 2 == k) & (z <= root) & (z > 0))
            def _():
                result_left(c).wait_send()

            @pl.when(((c + LOW // CHUNK) % 2 == k) & (z >= root) & (z < Z - 1))
            def _():
                result_right(c).wait_send()

    @pl.loop(0, groups)
    def _(g):
        for off in range(1, S):
            arrival(off, g).wait_recv()

    for spacing in [1 << t for t in range(2, count.bit_length() - 1)]:
        for i in range(spacing, count, 2 * spacing):
            whole[i] = whole[i] - 0.5 * (whole[i - spacing] + whole[(i + spacing) % count])

    def rs_right_copy(k, p):
        return remote(rs_send.at[k, p], rs_left.at[k, p], rs_ssem.at[k, p], rsl_recv.at[k, p], grid=lax.rem(z + 1, Z))

    def rs_left_copy(k, p):
        return remote(rs_send.at[k, p], rs_right.at[k, p], rs_ssem.at[k, p], rsr_recv.at[k, p],
                      grid=lax.rem(z + Z - 1, Z))

    def own(k, p, r):
        return whole[owner[k * owned + p * piece + r]]

    steps = (Z - 1) * pieces

    @pl.loop(0, steps + (Z - 1) * RS_LAG)
    def _(j):
        jr = j - RS_LAG * z
        inside_r = (jr >= 0) & (jr < steps)
        jr = jnp.clip(jr, 0, steps - 1)
        p = jr % pieces
        k = Z - 1 - jr // pieces

        @pl.when(inside_r & (k > z))
        def _():
            @pl.loop(0, piece)
            def _(r):
                rs_send[k, p, r] = own(k, p, r)

            @pl.when(z > 0)
            def _():
                rs_right_copy(k, p).wait_recv()

                @pl.loop(0, piece)
                def _(r):
                    rs_send[k, p, r] += rs_left[k, p, r]
            rs_right_copy(k, p).start()

        jl = j - RS_LAG * (Z - 1 - z)
        inside_l = (jl >= 0) & (jl < steps)
        jl = jnp.clip(jl, 0, steps - 1)
        q = jl % pieces
        n = jl // pieces

        @pl.when(inside_l & (n < z))
        def _():
            @pl.loop(0, piece)
            def _(r):
                rs_send[n, q, r] = own(n, q, r)

            @pl.when(z < Z - 1)
            def _():
                rs_left_copy(n, q).wait_recv()

                @pl.loop(0, piece)
                def _(r):
                    rs_send[n, q, r] += rs_right[n, q, r]
            rs_left_copy(n, q).start()

    @pl.loop(0, pieces)
    def _(p):
        @pl.loop(0, piece)
        def _(r):
            out[p * piece + r] = own(z, p, r)

        @pl.when(z > 0)
        def _():
            rs_right_copy(z, p).wait_recv()

            @pl.loop(0, piece)
            def _(r):
                out[p * piece + r] += rs_left[z, p, r]

        @pl.when(z < Z - 1)
        def _():
            rs_left_copy(z, p).wait_recv()

            @pl.loop(0, piece)
            def _(r):
                out[p * piece + r] += rs_right[z, p, r]

    @pl.loop(0, groups)
    def _(g):
        for off in range(1, S):
            exchange(off, g).wait_send()

    @pl.loop(0, Z)
    def _(k):
        @pl.when(k != z)
        def _():
            @pl.loop(0, pieces)
            def _(p):
                rs_right_copy(k, p).wait_send()


def local(field, levels, owner):
    _, rows, flat, lanes = field.shape
    Z, S = lax.axis_size("grid"), lax.axis_size("slab")
    count = owner.shape[0]
    tiles = flat // SUB
    tiles_out = tiles // S
    owned = count // Z
    piece = min(owned, 8)
    ext = rows + LOW + HIGH
    chunks = rows // CHUNK
    u = field[0].reshape(rows, tiles, SUB, lanes)
    tail = (tiles, SUB, lanes)
    tail_out = (tiles_out, SUB, lanes)
    f32 = jnp.float32
    vmem = lambda *shape: pltpu.VMEM(shape, f32)
    sems = lambda *shape: pltpu.SemaphoreType.DMA(shape)
    pieces = owned // piece
    result = pl.pallas_call(
        functools.partial(kernel, (Z, S, rows, count)),
        out_shape=jax.ShapeDtypeStruct((owned,) + tail_out, f32),
        in_specs=[pl.BlockSpec(memory_space=pltpu.SMEM), pl.BlockSpec(memory_space=pltpu.SMEM),
                  pl.BlockSpec(memory_space=pl.ANY)],
        out_specs=pl.BlockSpec(memory_space=pltpu.VMEM),
        scratch_shapes=[
            vmem(STEPS + 1, ext, *tail), vmem(STEPS + 1, ext, *tail), vmem(ext, *tail),
            vmem(rows, *tail), vmem(rows, *tail), vmem(rows, *tail),
            vmem(rows, *tail), vmem(count, *tail_out),
            vmem(Z, pieces, piece, *tail_out), vmem(Z, pieces, piece, *tail_out), vmem(Z, pieces, piece, *tail_out),
            sems(2), sems(2), sems(chunks), sems(chunks), sems(chunks), sems(chunks), sems(chunks), sems(chunks),
            sems(2), sems(2), sems(S - 1, rows // 4), sems(S - 1, rows // 4),
            sems(Z, pieces), sems(Z, pieces), sems(Z, pieces), pltpu.SemaphoreType.DMA,
        ],
        compiler_params=pltpu.CompilerParams(collective_id=0, has_side_effects=True,
                                             vmem_limit_bytes=40 * 1024 * 1024),
    )(levels, owner, u)
    return result.reshape(owned, flat // S, lanes)


def solution(mesh):
    in_specs = (P(("copies", "grid"), "slab", None, None), P(("copies", "grid"), None), P("copies"))
    out_specs = P(("copies", "grid"), "slab", None)
    return jax.shard_map(local, mesh=mesh, in_specs=in_specs, out_specs=out_specs, check_vma=False)
```
